32 devices in a mesh: exp: 8 (over y, x, core), tp: 4 (over z).
Axes of the slice: x: 2, y: 2, z: 4, core: 2. Of those that a mesh axis runs over, the one named last changes fastest.
Arguments:
- tokens: bfloat16 [224, 4096], P('exp', 'tp'), may hold values from -6 to 6
- cotangent: bfloat16 [224, 4096], P('exp', 'tp'), may hold values from -6 to 6
- experts: int32 [224, 2], P('exp'), may hold values from 0 to 7, all different within a row; in each aligned block of 28 rows (0 to 27, 28 to 55, ...) at most 8 rows name the same one
- gates: float32 [224, 2], P('exp'), may hold values from 0.1 to 0.9
- w_gate: bfloat16 [8, 4096, 8192], P('exp', None, 'tp'), may hold values from -0.09375 to 0.09375
- w_up: bfloat16 [8, 4096, 8192], P('exp', None, 'tp'), may hold values from -0.09375 to 0.09375
- w_down: bfloat16 [8, 8192, 4096], P('exp', 'tp'), may hold values from -0.0625 to 0.0625
Outputs:
- output: bfloat16 [224, 4096], P('exp', 'tp')
- input_grad: bfloat16 [224, 4096], P('exp', 'tp')
- grad_gate: bfloat16 [8, 4096, 8192], P('exp', None, 'tp')
- grad_up: bfloat16 [8, 4096, 8192], P('exp', None, 'tp')
- grad_down: bfloat16 [8, 8192, 4096], P('exp', 'tp')
The draws below stay inside these ranges and needn't reach their ends.
Inputs may be any that keep to these rules, and one draw needn't show every extreme that they name: Each row names 2 different experts. In each aligned block of 28 rows (the rows of one index of exp) no expert is named by more than 8 rows, and in some blocks one is named by exactly 8.
All inputs are finite; a program needn't handle non-finite values.
Results may differ from the reference program's by a relative error of at most 0.017.
Values may be sent and summed in bfloat16 or wider, within the bound.
A program may use at most 192 MiB of HBM per device.

```python
import math
import jax
import jax.numpy as jnp
import numpy as np
from jax import lax

D = 4096
FF = 8192
EXPERTS = 8
TOP = 2
TOK_DEV = 28
CAP = 8
GROUP = 1
TOKENS = 224
N_EXP = 8


def shard_levels(rng, shape, split, low, largest):
    gain = 1.0
    for dim, shards_of in split:
        draws = jax.random.uniform(jax.random.fold_in(jax.random.fold_in(rng, 6), dim), (shards_of,), jnp.float32, low / len(split), largest / len(split))
        gain = gain * jnp.repeat(jnp.exp(draws), shape[dim] // shards_of).reshape((-1,) + (1,) * (len(shape) - 1 - dim))
    return gain


def routed_block(rng, own, number, rows, count, top, most, slope):
    sequence = jax.random.permutation(rng, count)
    crowded, ordinary = load_shares(count, rows * top, most, slope, True), load_shares(count, rows * top, most, slope, False)
    places = jnp.arange(count)

    def named(lengths, turn):
        used = int((lengths > 0).sum())
        fixed = max(1, used // 4)
        moved = fixed + (places - fixed + turn * (used - fixed)) % max(1, count - fixed)
        return jnp.zeros((count,), jnp.int32).at[sequence[jnp.where(places < fixed, places, moved)]].set(jnp.asarray(lengths, jnp.int32))

    lengths = jnp.where(number % 4 == 0, named(crowded, number // 4), named(ordinary, number - number // 4 - 1))
    mixed = jax.random.permutation(jax.random.fold_in(own, 3), count)
    source_of, sink = mixed[0:count // 2 * 2:2], mixed[1:count // 2 * 2:2]
    room = jnp.minimum(lengths[source_of] - 1, most - lengths[sink]) // 2
    room = jnp.where((source_of == sequence[0]) | (sink == sequence[0]) | (lengths[sink] == 0), 0, jnp.maximum(room, 0))
    moved = jax.random.randint(jax.random.fold_in(own, 4), (count // 2,), 0, 1 << 20) % (room + 1)
    lengths = lengths.at[source_of].add(-moved).at[sink].add(moved)
    members = jnp.searchsorted(jnp.cumsum(lengths), jnp.arange(rows * top), side="right").astype(jnp.int32)
    listing = members.reshape(top, rows).T
    listing = listing[jax.random.permutation(jax.random.fold_in(own, 1), rows)]
    turn = jax.random.randint(jax.random.fold_in(own, 2), (rows, 1), 0, top)
    return jnp.take_along_axis(listing, (jnp.arange(top)[None, :] + turn) % top, axis=1)


def load_shares(count, total, bound, lean, full):
    weights = [(1 << 20) // math.isqrt(standing ** lean) + 1 for standing in range(1, count + 1)]
    largest = bound if full else min(bound, max(-(-total // count), total * weights[0] // sum(weights)))
    least = 1 if total - largest >= count - 1 else 0
    counts, rest = [largest] + [least] * (count - 1), total - largest - least * (count - 1)
    while rest > 0:
        free = [i for i in range(1, count) if counts[i] < largest] or [i for i in range(1, count) if counts[i] < bound]
        pool, budget = sum([weights[i] for i in free]), rest
        for i in free:
            more = min(bound - counts[i], max(1, budget * weights[i] // pool), rest)
            counts[i] = counts[i] + more
            rest = rest - more
    return np.array(counts)


def noise(key, extent, spread, most, split=(), kind=jnp.bfloat16):
    entries = jax.random.normal(key, extent, jnp.float32) * spread
    if len(split) > 0:
        entries = shard_levels(key, extent, split, -0.22, 0.18) * entries
    return jnp.clip(entries, min=-most, max=most).astype(kind)


def setup_inputs(seed: int = 0) -> dict:
    streams_of = jax.random.split(jax.random.key(seed), 8)
    tokens = noise(streams_of[0], (TOKENS, D), 1.0, 6.0, ((0, 8), (1, 4)))
    cotangent = noise(streams_of[1], (TOKENS, D), 1.0, 6.0, ((0, 8), (1, 4)))
    experts_keys = jax.random.split(jax.random.fold_in(streams_of[2], 1), TOKENS // TOK_DEV)
    experts_turns = jax.random.permutation(jax.random.fold_in(streams_of[2], 3), TOKENS // TOK_DEV)
    experts = jax.vmap(lambda own, number: routed_block(jax.random.fold_in(streams_of[2], 2), own, number, TOK_DEV, EXPERTS, TOP, CAP, 2))(experts_keys, experts_turns).reshape((TOKENS, TOP))
    gates = jnp.clip(0.1 + 0.79999997 * jax.random.uniform(streams_of[3], (TOKENS, TOP), jnp.float32) ** shard_levels(streams_of[3], (TOKENS, TOP), ((0, 8),), -0.2, 0.2), 0.1, 0.9)
    w_gate = noise(streams_of[4], (N_EXP, D, FF // GROUP), D ** -0.5, 0.09375, ((0, 8), (2, 4)))
    w_up = noise(streams_of[5], (N_EXP, D, FF // GROUP), D ** -0.5, 0.09375, ((0, 8), (2, 4)))
    w_down = noise(streams_of[6], (N_EXP, FF // GROUP, D), FF ** -0.5, 0.0625, ((0, 8), (1, 4)))
    return dict(tokens=tokens, cotangent=cotangent, experts=experts, gates=gates, w_gate=w_gate, w_up=w_up, w_down=w_down)


def slot_places(experts):
    pair_ids = experts.reshape(N_EXP, TOK_DEV * TOP)
    matches = (pair_ids[:, :, None] == jnp.arange(EXPERTS, dtype=jnp.int32)[None, None, :]).astype(jnp.int32)
    before = jnp.cumsum(matches, axis=1) - matches
    slot_ids = jnp.sum(before * matches, axis=2)
    source = jnp.arange(N_EXP, dtype=jnp.int32)[:, None] * CAP
    return (source + slot_ids).reshape(TOKENS * TOP).astype(jnp.int32)


def reference(tokens, cotangent, experts, gates, w_gate, w_up, w_down):
    places = slot_places(experts)
    expert_ids = experts.reshape(TOKENS * TOP).astype(jnp.int32)
    buffer_rows = N_EXP * CAP
    repeated = jnp.repeat(tokens, TOP, axis=0)
    scaled = (gates[:, :, None] * cotangent[:, None, :].astype(jnp.float32)).astype(jnp.bfloat16)
    scaled = scaled.reshape(TOKENS * TOP, D)
    part = FF // GROUP
    gate_all = w_gate.reshape(EXPERTS, GROUP, D, part).transpose(0, 2, 1, 3).reshape(EXPERTS, D, FF)
    up_all = w_up.reshape(EXPERTS, GROUP, D, part).transpose(0, 2, 1, 3).reshape(EXPERTS, D, FF)
    down_all = w_down.reshape(EXPERTS, FF, D)

    def expert_pass(expert):
        targets = jnp.where(expert_ids == expert, places, buffer_rows).astype(jnp.int32)
        token_rows = jnp.zeros((buffer_rows, D), jnp.bfloat16).at[targets].set(repeated, mode="drop")
        cot_rows = jnp.zeros((buffer_rows, D), jnp.bfloat16).at[targets].set(scaled, mode="drop")
        gate_mat = gate_all[expert]
        up_mat = up_all[expert]
        down_mat = down_all[expert]
        hidden_gate = jnp.dot(token_rows, gate_mat, preferred_element_type=jnp.float32)
        hidden_up = jnp.dot(token_rows, up_mat, preferred_element_type=jnp.float32)
        sigmoid_gate = jax.nn.sigmoid(hidden_gate)
        activation = (hidden_gate * sigmoid_gate * hidden_up).astype(jnp.bfloat16)
        out_rows = jnp.dot(activation, down_mat, preferred_element_type=jnp.float32)
        grad_act = jnp.dot(cot_rows, down_mat.T, preferred_element_type=jnp.float32)
        grad_first = (grad_act * hidden_up * sigmoid_gate * (1.0 + hidden_gate * (1.0 - sigmoid_gate))).astype(jnp.bfloat16)
        grad_second = (grad_act * hidden_gate * sigmoid_gate).astype(jnp.bfloat16)
        grad_down = jnp.dot(activation.T, cot_rows, preferred_element_type=jnp.float32).astype(jnp.bfloat16)
        grad_gate = jnp.dot(token_rows.T, grad_first, preferred_element_type=jnp.float32).astype(jnp.bfloat16)
        grad_up = jnp.dot(token_rows.T, grad_second, preferred_element_type=jnp.float32).astype(jnp.bfloat16)
        back_rows = jnp.dot(grad_first, gate_mat.T, preferred_element_type=jnp.float32)
        back_rows = back_rows + jnp.dot(grad_second, up_mat.T, preferred_element_type=jnp.float32)
        return out_rows, back_rows, grad_gate, grad_up, grad_down

    results = lax.map(expert_pass, jnp.arange(EXPERTS, dtype=jnp.int32))
    flat = (expert_ids * buffer_rows + places).astype(jnp.int32)
    out_pairs = results[0].reshape(EXPERTS * buffer_rows, D)[flat].reshape(TOKENS, TOP, D)
    back_pairs = results[1].reshape(EXPERTS * buffer_rows, D)[flat].reshape(TOKENS, TOP, D)
    output = jnp.sum(gates[:, :, None] * out_pairs, axis=1).astype(jnp.bfloat16)
    input_grad = jnp.sum(back_pairs, axis=1).astype(jnp.bfloat16)
    grad_gate = results[2].reshape(EXPERTS, D, GROUP, part).transpose(0, 2, 1, 3).reshape(N_EXP, D, part)
    grad_up = results[3].reshape(EXPERTS, D, GROUP, part).transpose(0, 2, 1, 3).reshape(N_EXP, D, part)
    grad_down = results[4].reshape(N_EXP, part, D)
    return output, input_grad, grad_gate, grad_up, grad_down
```

```python
import functools

import jax
import jax.numpy as jnp
from jax import lax
from jax.experimental import pallas as pl
from jax.experimental.pallas import tpu as pltpu
from jax.sharding import PartitionSpec as P

EXPERTS = 8
CAP = 8
MESH = pl.DeviceIdType.MESH


def contract_rows(left, right):
    return lax.dot_general(
        left, right, (((0,), (0,)), ((), ())), preferred_element_type=jnp.float32
    )


def contract_cols(left, right):
    return lax.dot_general(
        left, right, (((1,), (1,)), ((), ())), preferred_element_type=jnp.float32
    )


def slot_places(experts, capacity):
    pair_ids = experts.reshape(-1)
    matches = (pair_ids[:, None] == jnp.arange(EXPERTS, dtype=jnp.int32)[None, :]).astype(jnp.int32)
    before = jnp.cumsum(matches, axis=0) - matches
    slot_ids = jnp.sum(before * matches, axis=1)
    return pair_ids * capacity + slot_ids


def forward_kernel(n, m, group, bf, depth, send_ref, wg_hbm, wu_hbm, wd_hbm, *rest):
    x_ref, g_ref, a_ref, d1_ref, d3_ref = rest[:5]
    parts = rest[5 : 5 + m]
    (wg, wu, wd, w_sem, held, y_acc, b_acc, s1, r1, s2, r2) = rest[5 + m :]
    e, t = lax.axis_index("exp"), lax.axis_index("tp")
    cols = send_ref.shape[2]
    blocks = wg_hbm.shape[2] // bf

    def weight_copies(j, slot):
        span = pl.ds(pl.multiple_of(j * bf, bf), bf)
        return (
            pltpu.make_async_copy(wg_hbm.at[0, :, span], wg.at[slot], w_sem.at[slot, 0]),
            pltpu.make_async_copy(wu_hbm.at[0, :, span], wu.at[slot], w_sem.at[slot, 1]),
            pltpu.make_async_copy(wd_hbm.at[0, span, :], wd.at[slot], w_sem.at[slot, 2]),
        )

    barrier = pltpu.get_barrier_semaphore()
    for r in range(1, n):
        pl.semaphore_signal(
            barrier, inc=1, device_id={"exp": lax.rem(e + r, n), "tp": t}, device_id_type=MESH
        )
    for q in range(1, m):
        pl.semaphore_signal(
            barrier, inc=1, device_id={"exp": e, "tp": lax.rem(t + q, m)}, device_id_type=MESH
        )
    for j in range(depth):
        for copy in weight_copies(j, j):
            copy.start()
    pl.semaphore_wait(barrier, n - 1 + m - 1)

    def rows_of(source):
        return pl.ds(pl.multiple_of(source * 2 * CAP, 2 * CAP), 2 * CAP)

    def cols_of(part):
        return pl.ds(pl.multiple_of(part * cols, cols), cols)

    first = []
    for r in range(1, n):
        dest = lax.rem(e + r, n)
        copy = pltpu.make_async_remote_copy(
            src_ref=send_ref.at[dest // group],
            dst_ref=held.at[rows_of(e), cols_of(t)],
            send_sem=s1.at[r],
            recv_sem=r1.at[r],
            device_id={"exp": dest, "tp": t},
            device_id_type=MESH,
        )
        copy.start()
        first.append(copy)
    second = []
    for r in range(n):
        source = lax.rem(e - r + n, n)
        here = held.at[rows_of(source), cols_of(t)]
        if r > 0:
            first[r - 1].wait_recv()
        for q in range(1, m):
            copy = pltpu.make_async_remote_copy(
                src_ref=here if r > 0 else send_ref.at[e // group],
                dst_ref=here,
                send_sem=s2.at[r, q],
                recv_sem=r2.at[r, q],
                device_id={"exp": e, "tp": lax.rem(t + q, m)},
                device_id_type=MESH,
            )
            copy.start()
            second.append(copy)
    held[rows_of(e), cols_of(t)] = send_ref[e // group]
    y_acc[...] = jnp.zeros_like(y_acc)
    b_acc[...] = jnp.zeros_like(b_acc)
    for copy in second:
        copy.wait_recv()
    for part in range(m):
        span = pl.ds(part * cols, cols)
        pair = held[:, span].astype(jnp.float32).reshape(n, 2, CAP, cols)
        x_ref[:, span] = pair[:, 0].reshape(n * CAP, cols).astype(jnp.bfloat16)
        g_ref[:, span] = pair[:, 1].reshape(n * CAP, cols).astype(jnp.bfloat16)

    @pl.loop(0, blocks)
    def _(j):
        slot = lax.rem(j, depth)
        for copy in weight_copies(j, slot):
            copy.wait()
        span = pl.ds(pl.multiple_of(j * bf, bf), bf)
        h1 = jnp.dot(x_ref[...], wg[slot], preferred_element_type=jnp.float32)
        h3 = jnp.dot(x_ref[...], wu[slot], preferred_element_type=jnp.float32)
        da = contract_cols(g_ref[...], wd[slot])
        sig = jax.nn.sigmoid(h1)
        act = (h1 * sig * h3).astype(jnp.bfloat16)
        d1 = (da * h3 * sig * (1.0 + h1 * (1.0 - sig))).astype(jnp.bfloat16)
        d3 = (da * h1 * sig).astype(jnp.bfloat16)
        a_ref[:, span] = act
        d1_ref[:, span] = d1
        d3_ref[:, span] = d3
        y_acc[...] += jnp.dot(act, wd[slot], preferred_element_type=jnp.float32)
        b_acc[...] += contract_cols(d1, wg[slot]) + contract_cols(d3, wu[slot])

        @pl.when(j + depth < blocks)
        def _():
            for copy in weight_copies(j + depth, slot):
                copy.start()

    for r in range(m):
        span = cols_of(lax.rem(t + r, m))
        parts[r][0] = y_acc[:, span].astype(jnp.bfloat16)
        parts[r][1] = b_acc[:, span].astype(jnp.bfloat16)
    for copy in first + second:
        copy.wait_send()


def wide_kernel(x_ref, d1_ref, d3_ref, gate_ref, up_ref, xt):
    @pl.when(pl.program_id(0) == 0)
    def _():
        xt[...] = x_ref[...].astype(jnp.float32).T.astype(jnp.bfloat16)

    gate_ref[0] = jnp.dot(xt[...], d1_ref[...], preferred_element_type=jnp.float32).astype(
        jnp.bfloat16
    )
    up_ref[0] = jnp.dot(xt[...], d3_ref[...], preferred_element_type=jnp.float32).astype(
        jnp.bfloat16
    )


def sum_kernel(_, *rest):
    parts, out_ref = rest[:-1], rest[-1]
    total = parts[0][...].astype(jnp.float32)
    for part in parts[1:]:
        total = total + part[...].astype(jnp.float32)
    n, _, cap, cols = out_ref.shape
    for which in range(2):
        out_ref[:, which] = total[which].reshape(n, cap, cols).astype(out_ref.dtype)


def down_kernel(_, a_ref, g_ref, down_ref):
    down_ref[0] = contract_rows(a_ref[...], g_ref[...]).astype(jnp.bfloat16)


def per_device(tokens, cotangent, experts, gates, w_gate, w_up, w_down):
    n, m = lax.axis_size("exp"), lax.axis_size("tp")
    group = n // EXPERTS
    tok_rows, top_count = experts.shape
    width, hidden = w_gate.shape[1], w_gate.shape[2]
    cols = tokens.shape[1]
    rows = n * CAP
    bf = min(256, hidden)
    blocks = hidden // bf
    depth = min(6, blocks)

    places = slot_places(experts, CAP)
    pick = (
        places[:, None] == jnp.arange(EXPERTS * CAP, dtype=jnp.int32)[None, :]
    ).astype(jnp.float32)
    per_token = pick.reshape(tok_rows, top_count, EXPERTS * CAP)
    weighted = jnp.sum(per_token * gates[:, :, None], axis=1)
    unweighted = jnp.sum(per_token, axis=1)
    row_gate = jnp.sum(weighted, axis=0)
    pick_low = unweighted.astype(jnp.bfloat16)
    both = jnp.concatenate([tokens, cotangent], axis=1)
    picked = contract_rows(pick_low, both)
    token_rows = picked[:, :cols].astype(jnp.bfloat16)
    scaled = (picked[:, cols:] * row_gate[:, None]).astype(jnp.bfloat16)
    send = jnp.concatenate(
        [token_rows.reshape(EXPERTS, CAP, cols), scaled.reshape(EXPERTS, CAP, cols)], axis=1
    )

    vmem = pl.BlockSpec(memory_space=pltpu.VMEM)
    anyw = pl.BlockSpec(memory_space=pl.ANY)
    low = jnp.bfloat16
    wide = jax.ShapeDtypeStruct((rows, width), low)
    narrow = jax.ShapeDtypeStruct((rows, hidden), low)
    part = jax.ShapeDtypeStruct((2, rows, cols), low)
    outs = pl.pallas_call(
        functools.partial(forward_kernel, n, m, group, bf, depth),
        out_shape=[wide, wide, narrow, narrow, narrow] + [part] * m,
        in_specs=[vmem, anyw, anyw, anyw],
        out_specs=[vmem] * (5 + m),
        scratch_shapes=[
            pltpu.VMEM((depth, width, bf), low),
            pltpu.VMEM((depth, width, bf), low),
            pltpu.VMEM((depth, bf, width), low),
            pltpu.SemaphoreType.DMA((depth, 3)),
            pltpu.VMEM((2 * rows, width), low),
            pltpu.VMEM((rows, width), jnp.float32),
            pltpu.VMEM((rows, width), jnp.float32),
            pltpu.SemaphoreType.DMA((n,)),
            pltpu.SemaphoreType.DMA((n,)),
            pltpu.SemaphoreType.DMA((n, m)),
            pltpu.SemaphoreType.DMA((n, m)),
        ],
        compiler_params=pltpu.CompilerParams(
            collective_id=0, has_side_effects=True, vmem_limit_bytes=60 * 1024 * 1024
        ),
        cost_estimate=pl.CostEstimate(
            flops=12 * rows * width * hidden,
            bytes_accessed=6 * width * hidden,
            transcendentals=rows * hidden,
        ),
        name="forward",
    )(send, w_gate, w_up, w_down)
    x, g, act, d1, d3 = outs[:5]
    parts = outs[5:]

    got = [
        lax.ppermute(parts[r], "tp", [(i, (i + r) % m) for i in range(m)]) for r in range(1, m)
    ]

    gb = min(256, hidden)
    full = pl.BlockSpec((rows, width), lambda j: (0, 0))
    strip = pl.BlockSpec((rows, gb), lambda j: (0, j))
    grad_gate, grad_up = pl.pallas_call(
        wide_kernel,
        out_shape=[jax.ShapeDtypeStruct(w_gate.shape, low)] * 2,
        grid=(hidden // gb,),
        in_specs=[full, strip, strip],
        out_specs=[pl.BlockSpec((1, width, gb), lambda j: (0, 0, j))] * 2,
        scratch_shapes=[pltpu.VMEM((width, rows), low)],
        compiler_params=pltpu.CompilerParams(
            dimension_semantics=("arbitrary",), vmem_limit_bytes=40 * 1024 * 1024
        ),
        cost_estimate=pl.CostEstimate(
            flops=4 * rows * width * hidden, bytes_accessed=4 * width * hidden, transcendentals=0
        ),
        name="grad_wide",
    )(x, d1, d3)
    total = pl.pallas_call(
        sum_kernel,
        out_shape=jax.ShapeDtypeStruct((n, 2, CAP, cols), low),
        in_specs=[anyw] + [vmem] * m,
        out_specs=vmem,
        name="sum_parts",
    )(grad_gate, parts[0], *got)
    grad_down = pl.pallas_call(
        down_kernel,
        out_shape=jax.ShapeDtypeStruct(w_down.shape, low),
        grid=(hidden // gb,),
        in_specs=[anyw, strip, full],
        out_specs=pl.BlockSpec((1, gb, width), lambda j: (0, j, 0)),
        compiler_params=pltpu.CompilerParams(
            dimension_semantics=("arbitrary",), vmem_limit_bytes=40 * 1024 * 1024
        ),
        cost_estimate=pl.CostEstimate(
            flops=2 * rows * width * hidden, bytes_accessed=2 * width * hidden, transcendentals=0
        ),
        name="grad_down",
    )(total, act, g)

    back = lax.all_to_all(total, "exp", split_axis=0, concat_axis=0, tiled=True)
    back = back.astype(jnp.float32).reshape(EXPERTS, group, 2, CAP, cols)
    back = jnp.sum(back, axis=1).transpose(1, 0, 2, 3).reshape(2, EXPERTS * CAP, cols)

    def combine(table, values):
        return jnp.dot(
            table, values, precision=lax.Precision.HIGHEST, preferred_element_type=jnp.float32
        ).astype(low)

    return (
        combine(weighted, back[0]),
        combine(unweighted, back[1]),
        grad_gate,
        grad_up,
        grad_down,
    )


def solution(mesh):
    in_specs = (
        P("exp", "tp"),
        P("exp", "tp"),
        P("exp", None),
        P("exp", None),
        P("exp", None, "tp"),
        P("exp", None, "tp"),
        P("exp", "tp", None),
    )
    out_specs = (
        P("exp", "tp"),
        P("exp", "tp"),
        P("exp", None, "tp"),
        P("exp", None, "tp"),
        P("exp", "tp", None),
    )
    return jax.shard_map(
        per_device, mesh=mesh, in_specs=in_specs, out_specs=out_specs, check_vma=False
    )
```
